32 devices in a mesh: blk: 8 (over z, x), col: 4 (over y, core).
Axes of the slice: x: 2, y: 2, z: 4, core: 2. Of those that a mesh axis runs over, the one named last changes fastest.
Arguments:
- pixel_row: int32 [2048, 256], P(('blk', 'col')), may hold values from 0 to 63, as said below
- pixel_col: int32 [2048, 256], P(('blk', 'col')), may hold values from 0 to 2047, as said below
- strip_of_span: int32 [32, 64], P(('blk', 'col')), may hold values from 0 to 31, as said below
- shear_one: float32 [2048, 256], P(('blk', 'col')), may hold values from -6 to 6
- shear_two: float32 [2048, 256], P(('blk', 'col')), may hold values from -6 to 6
- weight: float32 [2048, 256], P(('blk', 'col')), may hold values from 0.25 to 4
Outputs:
- kappa_e: float32 [2048, 8192], P(('blk', 'col'))
- kappa_b: float32 [2048, 8192], P(('blk', 'col'))
The draws below stay inside these ranges and needn't reach their ends.
Inputs may be any that keep to these rules, and one draw needn't show every extreme that they name: `pixel_row`: all galaxies of one span (one row) lie in one aligned band of 8 rows. `pixel_col`: all galaxies of one span (one row) lie in one aligned block of 128 columns. `strip_of_span`: row d names the row strip of each span of shard d; each strip is named exactly 2 times in every row.
All inputs are finite; a program needn't handle non-finite values.
Results may differ from the reference program's by a relative error of at most 0.0038.
Values may be sent and summed in bfloat16 or wider, within the bound.
A program may use at most 128 MiB of HBM per device.

```python
import math
import jax
import jax.numpy as jnp
from jax import lax

SLAB = 256
TILE_COLS = 2048
BAND = 8
SUBC = 128
GAL = 256
DEPTH = 2
STRIP = 64
SHARD_SPANS = 64
SPANS = 2048
N_BLK = 8
N_COL = 4


def draw_pixel_row(key, part):
    band_key, offset_key = jax.random.split(jax.random.fold_in(key, 11))
    band_pick = jax.random.randint(band_key, (SPANS, 1), 0, STRIP // BAND)
    offsets = jax.random.randint(offset_key, (SPANS, GAL), 0, BAND)
    return (band_pick * BAND + offsets).astype(jnp.int32)


def draw_pixel_col(key, part):
    block_key, offset_key = jax.random.split(jax.random.fold_in(key, 23))
    blocks = jax.random.randint(block_key, (SPANS, 1), 0, TILE_COLS // SUBC)
    offsets = jax.random.randint(offset_key, (SPANS, GAL), 0, SUBC)
    return (blocks * SUBC + offsets).astype(jnp.int32)


def draw_strip_of_span(key, part):
    row_keys = jax.random.split(jax.random.fold_in(key, 31), N_BLK * N_COL)
    orders = jax.vmap(lambda one_key: jax.random.permutation(one_key, SHARD_SPANS))(row_keys)
    return (orders % (SHARD_SPANS // DEPTH)).astype(jnp.int32)


def block_levels(own_key, dims, pieces, least, top_value):
    loudness = 1.0
    for position, blocks in pieces:
        draws = jax.random.uniform(jax.random.fold_in(jax.random.fold_in(own_key, 6), position), (blocks,), jnp.float32, least / len(pieces), top_value / len(pieces))
        loudness = loudness * jnp.repeat(jnp.exp(draws), dims[position] // blocks).reshape((-1,) + (1,) * (len(dims) - 1 - position))
    return loudness


def gaussian(stream_key, shape, width, most, shards=(), kind=jnp.bfloat16):
    entries = jax.random.normal(stream_key, shape, jnp.float32) * width
    if len(shards) > 0:
        entries = block_levels(stream_key, shape, shards, -0.22, 0.18) * entries
    return jnp.clip(entries, min=-most, max=most).astype(kind)


def setup_inputs(seed: int = 0) -> dict:
    seeds = jax.random.split(jax.random.key(seed), 7)
    return {
        "pixel_row": draw_pixel_row(jax.random.fold_in(seeds[6], 71), 0),
        "pixel_col": draw_pixel_col(jax.random.fold_in(seeds[6], 71), 0),
        "strip_of_span": draw_strip_of_span(jax.random.fold_in(seeds[6], 71), 0),
        "shear_one": gaussian(seeds[3], (SPANS, GAL), 1.0, 6.0, ((0, 32),), jnp.float32),
        "shear_two": gaussian(seeds[4], (SPANS, GAL), 1.0, 6.0, ((0, 32),), jnp.float32),
        "weight": jnp.clip(jnp.exp(math.log(4.0) - 2.7725887 * jax.random.uniform(seeds[5], (SPANS, GAL), jnp.float32) ** block_levels(seeds[5], (SPANS, GAL), ((0, 32),), -0.2, 0.2)), 0.25, 4.0),
    }


def reference(pixel_row, pixel_col, strip_of_span, shear_one, shear_two, weight):
    span_count = pixel_row.shape[0]
    map_rows = SLAB * N_BLK
    map_cols = TILE_COLS * N_COL
    shard_size = strip_of_span.shape[1]
    shard_index = jnp.arange(span_count, dtype=jnp.int32) // shard_size
    strip_index = strip_of_span.reshape(-1).astype(jnp.int32)
    grid_row = strip_index[:, None] * STRIP + pixel_row
    grid_col = (shard_index % N_COL)[:, None] * TILE_COLS + pixel_col
    cell = (grid_row * map_cols + grid_col).astype(jnp.int32).reshape(-1)
    rounded_weight = lax.optimization_barrier(weight.astype(jnp.bfloat16)).astype(jnp.float32).reshape(-1)
    weighted_one = lax.optimization_barrier((weight * shear_one).astype(jnp.bfloat16)).astype(jnp.float32).reshape(-1)
    weighted_two = lax.optimization_barrier((weight * shear_two).astype(jnp.bfloat16)).astype(jnp.float32).reshape(-1)
    zeros_cells = jnp.zeros((map_rows * map_cols,), jnp.float32)
    weight_sum = zeros_cells.at[cell].add(rounded_weight)
    sum_one = zeros_cells.at[cell].add(weighted_one)
    sum_two = zeros_cells.at[cell].add(weighted_two)
    floored = jnp.maximum(weight_sum, 1.0)
    gamma_one = (sum_one / floored).reshape(map_rows, map_cols)
    gamma_two = (sum_two / floored).reshape(map_rows, map_cols)
    spectrum = jnp.fft.fft2(lax.complex(gamma_one, gamma_two))
    freq_x = jnp.fft.fftfreq(map_cols).astype(jnp.float32)[None, :]
    freq_y = jnp.fft.fftfreq(map_rows).astype(jnp.float32)[:, None]
    radius_sq = freq_x * freq_x + freq_y * freq_y
    safe_radius = jnp.where(radius_sq > 0, radius_sq, 1.0)
    kernel_re = (freq_x * freq_x - freq_y * freq_y) / safe_radius
    kernel_im = 2.0 * freq_x * freq_y / safe_radius
    spec_re = jnp.real(spectrum)
    spec_im = jnp.imag(spectrum)
    hat_re = kernel_re * spec_re + kernel_im * spec_im
    hat_im = kernel_re * spec_im - kernel_im * spec_re
    convergence = jnp.fft.ifft2(lax.complex(hat_re, hat_im))
    return jnp.real(convergence).astype(jnp.float32), jnp.imag(convergence).astype(jnp.float32)
```

```python
import math

import jax
import jax.numpy as jnp
import numpy as np
from jax import lax
from jax.experimental import pallas as pl
from jax.experimental.pallas import tpu as pltpu
from jax.sharding import PartitionSpec as P

SLAB = 256
TILE_COLS = 2048
BAND = 8
SUBC = 128
DEPTH = 2


highest = lax.Precision.HIGHEST
MESH = pl.DeviceIdType.MESH


def factor_pair(length):
    return (length // 128, 128)


def complex_table(left_len, right_len, modulus, direction):
    first_idx = lax.broadcasted_iota(jnp.int32, (left_len, right_len), 0)
    second_idx = lax.broadcasted_iota(jnp.int32, (left_len, right_len), 1)
    angles = (
        direction * 2.0 * math.pi / modulus * (first_idx * second_idx % modulus).astype(jnp.float32)
    )
    cosine = jnp.cos(angles)
    sine_part = jnp.sin(angles)
    return jnp.stack([jnp.stack([cosine, sine_part], -1), jnp.stack([-sine_part, cosine], -1)], 0)


def twiddle_parts(outer_len, inner_len, modulus, direction, factor):
    first_idx = lax.broadcasted_iota(jnp.int32, (outer_len, inner_len), 0)
    second_idx = lax.broadcasted_iota(jnp.int32, (outer_len, inner_len), 1)
    angles = (
        direction * 2.0 * math.pi / modulus * (first_idx * second_idx % modulus).astype(jnp.float32)
    )
    return (factor * jnp.cos(angles), factor * jnp.sin(angles))


def rotate(complex_field, cosine, sine_part):
    return jnp.stack(
        [
            complex_field[0] * cosine - complex_field[1] * sine_part,
            complex_field[0] * sine_part + complex_field[1] * cosine,
        ]
    )


def transform_rows(complex_field, direction):
    row_count = complex_field.shape[1]
    length = complex_field.shape[2]
    outer_len, inner_len = factor_pair(length)
    factor = 1.0 if direction < 0 else 1.0 / length
    cosine, sine_part = twiddle_parts(outer_len, inner_len, length, direction, factor)
    small_table = complex_table(outer_len, outer_len, outer_len, direction)
    large_table = complex_table(inner_len, inner_len, inner_len, direction)
    blocked = complex_field.reshape(2, row_count, outer_len, inner_len)
    if direction < 0:
        blocked = jnp.einsum("prab,pakq->qrkb", blocked, small_table, precision=highest)
        blocked = rotate(blocked, cosine, sine_part)
        blocked = jnp.einsum("prkb,pbsq->qrks", blocked, large_table, precision=highest)
    else:
        blocked = jnp.einsum("prks,psbq->qrkb", blocked, large_table, precision=highest)
        blocked = rotate(blocked, cosine, sine_part)
        blocked = jnp.einsum("prkb,pkaq->qrab", blocked, small_table, precision=highest)
    return blocked.reshape(2, row_count, length)


def transform_columns(complex_field, direction):
    length = complex_field.shape[1]
    col_count = complex_field.shape[2]
    outer_len, inner_len = factor_pair(length)
    factor = 1.0 if direction < 0 else 1.0 / length
    cosine, sine_part = twiddle_parts(outer_len, inner_len, length, direction, factor)
    cosine = cosine[:, :, None]
    sine_part = sine_part[:, :, None]
    small_table = complex_table(outer_len, outer_len, outer_len, direction)
    large_table = complex_table(inner_len, inner_len, inner_len, direction)
    blocked = complex_field.reshape(2, outer_len, inner_len, col_count)
    if direction < 0:
        blocked = jnp.einsum("pabw,pakq->qkbw", blocked, small_table, precision=highest)
        blocked = rotate(blocked, cosine, sine_part)
        blocked = jnp.einsum("pkbw,pbsq->qksw", blocked, large_table, precision=highest)
    else:
        blocked = jnp.einsum("pksw,psbq->qkbw", blocked, large_table, precision=highest)
        blocked = rotate(blocked, cosine, sine_part)
        blocked = jnp.einsum("pkbw,pkaq->qabw", blocked, small_table, precision=highest)
    return blocked.reshape(2, length, col_count)


def signed_frequency(position, length):
    outer_len, inner_len = factor_pair(length)
    freq_index = position // inner_len + outer_len * (position % inner_len)
    signed = jnp.where(freq_index < length // 2, freq_index, freq_index - length)
    return signed.astype(jnp.float32) / length


def bin_region(rows_in, cols_in, values, region_rows, region_cols):
    span_count = rows_in.shape[0]
    galaxies = rows_in.shape[1]
    band_count = region_rows // BAND
    blocks = region_cols // SUBC
    position = rows_in[:, 0] // BAND * blocks + cols_in[:, 0] // SUBC
    group_size = math.gcd(span_count, 128)

    def one_group(unused, group_data):
        row_part, col_part, value_part = group_data
        row_hot = (row_part[:, None, :] == lax.broadcasted_iota(jnp.int32, (1, BAND, 1), 1)).astype(
            jnp.bfloat16
        )
        weighted = (value_part[:, :, None, :] * row_hot[:, None, :, :]).reshape(
            group_size, 3 * BAND, galaxies
        )
        col_hot = (col_part[:, :, None] == lax.broadcasted_iota(jnp.int32, (1, 1, SUBC), 2)).astype(
            jnp.bfloat16
        )
        return (
            unused,
            jnp.einsum("ckg,cgs->cks", weighted, col_hot, preferred_element_type=jnp.float32),
        )

    group_inputs = (
        (rows_in % BAND).reshape(-1, group_size, galaxies),
        (cols_in % SUBC).reshape(-1, group_size, galaxies),
        values.reshape(-1, group_size, 3, galaxies),
    )
    unused_carry, partials = lax.scan(one_group, jnp.zeros((), jnp.float32), group_inputs)
    partials = partials.reshape(span_count, 3 * BAND * SUBC)
    summed = jax.ops.segment_sum(partials, position, num_segments=band_count * blocks)
    summed = summed.reshape(band_count, blocks, 3, BAND, SUBC).transpose(2, 0, 3, 1, 4)
    summed = summed.reshape(3, region_rows, region_cols)
    floored = jnp.maximum(summed[0], 1.0)
    return jnp.stack([summed[1] / floored, summed[2] / floored])


def generic_local(pixel_row, pixel_col, strip_of_span, shear_one, shear_two, weight):
    tile_count = lax.axis_size("col")
    my_slab = lax.axis_index("blk")
    my_tile = lax.axis_index("col")
    strip_rows = SLAB // tile_count
    span_total = pixel_row.shape[0]
    by_strip = jnp.argsort(strip_of_span[0], stable=True)
    packed = jnp.take(pixel_row * TILE_COLS + pixel_col, by_strip, axis=0)
    values = jnp.stack(
        [
            weight.astype(jnp.bfloat16),
            (weight * shear_one).astype(jnp.bfloat16),
            (weight * shear_two).astype(jnp.bfloat16),
        ],
        axis=1,
    )
    values = jnp.take(values, by_strip, axis=0)
    arrival = jnp.arange(span_total, dtype=jnp.int32) // DEPTH
    own_cell, own_values = (
        lax.all_to_all(packed, ("blk", "col"), split_axis=0, concat_axis=0, tiled=True),
        lax.all_to_all(values, ("blk", "col"), split_axis=0, concat_axis=0, tiled=True),
    )
    rows_in = own_cell // TILE_COLS
    cols_in = (arrival % tile_count)[:, None] * TILE_COLS + own_cell % TILE_COLS
    whole_rows = bin_region(rows_in, cols_in, own_values, strip_rows, TILE_COLS * tile_count)
    row_spectrum = transform_rows(whole_rows, -1)
    total_cols = row_spectrum.shape[2]
    whole_cols = lax.all_to_all(
        row_spectrum, ("blk", "col"), split_axis=2, concat_axis=1, tiled=True
    )
    col_width = whole_cols.shape[2]
    first_col = (my_slab * tile_count + my_tile) * col_width
    spectrum = transform_columns(whole_cols, -1)
    total_rows = spectrum.shape[1]
    freq_y = signed_frequency(jnp.arange(total_rows, dtype=jnp.int32), total_rows)[:, None]
    freq_x = signed_frequency(first_col + jnp.arange(col_width, dtype=jnp.int32), total_cols)[
        None, :
    ]
    radius_sq = freq_x * freq_x + freq_y * freq_y
    safe_radius = jnp.where(radius_sq > 0, radius_sq, 1.0)
    kernel_re = (freq_x * freq_x - freq_y * freq_y) / safe_radius
    kernel_im = 2.0 * freq_x * freq_y / safe_radius
    kappa_hat = jnp.stack(
        [
            kernel_re * spectrum[0] + kernel_im * spectrum[1],
            kernel_re * spectrum[1] - kernel_im * spectrum[0],
        ]
    )
    col_result = transform_columns(kappa_hat, 1)
    back_rows = lax.all_to_all(col_result, ("blk", "col"), split_axis=1, concat_axis=2, tiled=True)
    convergence = transform_rows(back_rows, 1)
    return (convergence[0], convergence[1])


LANES = 128
CHANNELS = 6
VMEM_BYTES = 60 * 1024 * 1024


def split_hi_lo(x):
    hi = x.astype(jnp.bfloat16)
    return hi, (x - hi.astype(jnp.float32)).astype(jnp.bfloat16)


def fft_list(points, sign):
    n = len(points)
    if n == 1:
        return points
    even = fft_list(points[0::2], sign)
    odd = fft_list(points[1::2], sign)
    half = n // 2
    first, second = [], []
    root = math.sqrt(0.5)
    for k in range(half):
        er, ei = even[k]
        r, i = odd[k]
        if k == 0:
            tr, ti = r, i
            first.append((er + tr, ei + ti))
            second.append((er - tr, ei - ti))
            continue
        if 4 * k == n:
            if sign > 0:
                first.append((er - i, ei + r))
                second.append((er + i, ei - r))
            else:
                first.append((er + i, ei - r))
                second.append((er - i, ei + r))
            continue
        if 8 * k == n:
            tr, ti = (root * (r - sign * i), root * (i + sign * r)) if sign > 0 else (
                root * (r + i), root * (i - r))
        elif 8 * k == 3 * n:
            tr, ti = (-root * (r + i), root * (r - i)) if sign > 0 else (
                root * (i - r), -root * (r + i))
        else:
            c = math.cos(2 * math.pi * k / n)
            s = sign * math.sin(2 * math.pi * k / n)
            tr, ti = r * c - i * s, r * s + i * c
        first.append((er + tr, ei + ti))
        second.append((er - tr, ei - ti))
    return first + second


def np_real_form(length, direction, factor, transposed):
    idx = np.arange(length)
    ang = direction * 2 * np.pi / length * (np.outer(idx, idx) % length)
    c, s = factor * np.cos(ang), factor * np.sin(ang)
    full = np.block([[c, s], [-s, c]])
    full = (full.T if transposed else full).astype(np.float32)
    hi = full.astype(jnp.bfloat16)
    lo = (full - hi.astype(np.float32)).astype(jnp.bfloat16)
    return np.stack([hi, lo])


def np_twiddle(outer, inner, direction):
    ang = direction * 2 * np.pi / (outer * inner) * np.outer(np.arange(outer), np.arange(inner))
    return np.cos(ang).astype(np.float32), np.sin(ang).astype(np.float32)


def side_tables(outer):
    quarter = outer // 4
    pre = np.zeros((2, 2, quarter, 2), np.float32)
    tw = np.zeros((2, outer, LANES), np.float32)
    for side in range(2):
        for parity in range(2):
            residue = 2 * side + parity
            ang = -2 * np.pi * residue * np.arange(quarter) / outer
            pre[side, parity, :, 0], pre[side, parity, :, 1] = np.cos(ang), np.sin(ang)
            k = 4 * np.arange(quarter) + residue
            ang = -2 * np.pi / (outer * LANES) * np.outer(k, np.arange(LANES))
            at = parity * quarter
            tw[side, at : at + quarter] = np.cos(ang)
            tw[side, 2 * quarter + at : 2 * quarter + at + quarter] = np.sin(ang)
    return pre.reshape(-1), tw


def dot(a, b):
    return jnp.dot(a, b, preferred_element_type=jnp.float32)


def pack_kernel(row_ref, col_ref, strip_ref, one_ref, two_ref, weight_ref, out_ref, *, depth):
    spans = row_ref.shape[0]
    gal = row_ref.shape[1]
    strip_row = strip_ref[...]
    lane = lax.broadcasted_iota(jnp.int32, (spans, spans), 1)
    sub = lax.broadcasted_iota(jnp.int32, (spans, spans), 0)
    wide = jnp.broadcast_to(strip_row, (spans, spans))
    strip_col = jnp.sum(jnp.where(lane == sub, wide, 0), axis=1, keepdims=True)
    earlier = jnp.where((wide == strip_col) & (sub < lane), 1, 0)
    slot = strip_row * depth + jnp.sum(earlier, axis=0, keepdims=True)
    perm = jnp.where(slot == sub, 1.0, 0.0).astype(jnp.bfloat16)
    w = weight_ref[...]
    r = row_ref[...]
    c = col_ref[...]
    tile_blocks = TILE_COLS // SUBC
    pieces = (
        w.astype(jnp.bfloat16),
        (w * one_ref[...]).astype(jnp.bfloat16),
        (w * two_ref[...]).astype(jnp.bfloat16),
        (r % BAND).astype(jnp.float32).astype(jnp.bfloat16),
        (c % SUBC).astype(jnp.float32).astype(jnp.bfloat16),
        ((r // BAND) * tile_blocks + c // SUBC).astype(jnp.float32).astype(jnp.bfloat16),
    )
    for n, piece in enumerate(pieces):
        sorted_piece = dot(perm, piece).astype(jnp.bfloat16)
        out_ref[:spans, n * gal : (n + 1) * gal] = sorted_piece
        out_ref[spans:, n * gal : (n + 1) * gal] = sorted_piece


def rows_kernel(
    block_ref, band_ref, side_ref, pre_ref, spans_ref, tw_ref, table_ref, even_ref, odd_ref,
    spans32, acc, mid,
):
    spans = spans_ref.shape[0]
    gal = spans_ref.shape[1] // CHANNELS
    outer, rows = acc.shape[1], acc.shape[2]
    spans32[...] = spans_ref[...].astype(jnp.float32)

    def clear(a, carry):
        acc[:, a] = jnp.zeros((3, rows, LANES), jnp.float32)
        return carry

    lax.fori_loop(0, outer, clear, 0)
    band_iota = lax.broadcasted_iota(jnp.int32, (BAND, gal), 0).astype(jnp.float32)
    col_iota = lax.broadcasted_iota(jnp.int32, (SUBC, gal), 0).astype(jnp.float32)

    def one_span(j, carry):
        part = lambda n: spans32[pl.ds(j, 1), n * gal : (n + 1) * gal]
        hot = part(3) == band_iota
        weighted = jnp.concatenate(
            [jnp.where(hot, part(n), 0.0) for n in range(3)], axis=0
        ).astype(jnp.bfloat16)
        col_hot = jnp.where(part(4) == col_iota, 1.0, 0.0).astype(jnp.bfloat16)
        cells = lax.dot_general(
            weighted, col_hot, (((1,), (1,)), ((), ())), preferred_element_type=jnp.float32
        )
        a = block_ref[j]
        at = pl.ds(pl.multiple_of(band_ref[j] * BAND, BAND), BAND)
        for n in range(3):
            acc[n, a, at, :] += cells[n * BAND : (n + 1) * BAND]
        return carry

    lax.fori_loop(0, spans, one_span, 0, unroll=4)

    half = outer // 4
    side = side_ref[0]
    sign = (1 - 2 * side).astype(jnp.float32)

    def chunk(rc, carry):
        at = pl.ds(pl.multiple_of(rc * 8, 8), 8)
        points = ([], [])
        for a in range(half):
            x = []
            for c in range(4):
                inv = 1.0 / jnp.maximum(acc[0, a + c * half, at, :], 1.0)
                x.append((acc[1, a + c * half, at, :] * inv, acc[2, a + c * half, at, :] * inv))
            sum_r, sum_i = sign * (x[1][0] + x[3][0]), sign * (x[1][1] + x[3][1])
            dif_r, dif_i = sign * (x[1][0] - x[3][0]), sign * (x[1][1] - x[3][1])
            whole = (
                (x[0][0] + x[2][0] + sum_r, x[0][1] + x[2][1] + sum_i),
                (x[0][0] - x[2][0] + dif_i, x[0][1] - x[2][1] - dif_r),
            )
            for parity, (re, im) in enumerate(whole):
                base = ((side * 2 + parity) * half + a) * 2
                c, s = pre_ref[base], pre_ref[base + 1]
                points[parity].append((re * c - im * s, re * s + im * c))
        for parity in range(2):
            for m, (re, im) in enumerate(fft_list(points[parity], -1)):
                slot = parity * half + m
                c = tw_ref[side, slot : slot + 1, :]
                s = tw_ref[side, 2 * half + slot : 2 * half + slot + 1, :]
                mid[slot, at, :LANES] = re * c - im * s
                mid[slot, at, LANES:] = re * s + im * c
        return carry

    lax.fori_loop(0, rows // 8, chunk, 0)
    group = math.gcd(half, 4)
    for parity, out_ref in enumerate((even_ref, odd_ref)):

        def matmul(g, carry):
            hi, lo = split_hi_lo(
                mid[pl.ds(parity * half + g * group, group)].reshape(group * rows, 2 * LANES)
            )
            th, tl = table_ref[0], table_ref[1]
            res = dot(hi, th) + (dot(lo, th) + dot(hi, tl))
            out_ref[pl.ds(g * group, group)] = res.astype(jnp.bfloat16).reshape(
                group, rows, 2 * LANES
            )
            return carry

        lax.fori_loop(0, half // group, matmul, 0)


def cols_transform(in_ref, tw_ref, fwd_ref, inv_ref, out_ref, mid, first, total_cols, outer_cols):
    rows = in_ref.shape[1]
    out_rows = out_ref.shape[1]
    outer = 2 * mid.shape[0]
    inner = mid.shape[1] // 2
    per = inner // rows
    out_per = inner // out_rows
    total_rows = outer * inner
    step = 16
    chunks = rows // step
    out_chunks = out_rows // step

    def place(t):
        h = t // chunks
        at = pl.ds(pl.multiple_of((t % chunks) * step, step), step)
        re_at = pl.ds(pl.multiple_of(t * step, step), step)
        im_at = pl.ds(pl.multiple_of(inner + t * step, step), step)
        return h, at, re_at, im_at

    def lanes(n):
        return slice(n % 2 * LANES, (n % 2 + 1) * LANES)

    def forward(t, carry):
        h, at, re_at, im_at = place(t)
        points = []
        for a in range(outer):
            both = in_ref[a * per + h, at, :].astype(jnp.float32)
            points.append((both[:, :LANES], both[:, LANES:]))
        for n, (re, im) in enumerate(fft_list(points, -1)):
            c = tw_ref[re_at, n : n + 1]
            s = tw_ref[re_at, outer + n : outer + n + 1]
            mid[n // 2, re_at, lanes(n)] = re * c - im * s
            mid[n // 2, im_at, lanes(n)] = re * s + im * c
        return carry

    lax.fori_loop(0, inner // step, forward, 0)

    lane = lax.broadcasted_iota(jnp.int32, (1, 2 * LANES), 1)
    v = first + outer_cols * (lane % LANES)
    fx = jnp.where(v < total_cols // 2, v, v - total_cols).astype(jnp.float32) / total_cols

    def middle(n, carry):
        hi, lo = split_hi_lo(mid[n])
        th, tl = fwd_ref[0], fwd_ref[1]
        spec = dot(th, hi) + (dot(tl, hi) + dot(th, lo))
        sr, si = spec[:inner], spec[inner:]
        u = 2 * n + lane // LANES + outer * lax.broadcasted_iota(
            jnp.int32, (inner, 2 * LANES), 0
        )
        fy = jnp.where(u < total_rows // 2, u, u - total_rows).astype(jnp.float32) / total_rows
        fx2, fy2 = fx * fx, fy * fy
        radius = fx2 + fy2
        inv_radius = 1.0 / jnp.where(radius > 0, radius, 1.0)
        kr = (fx2 - fy2) * inv_radius
        ki = (2.0 * fx) * fy * inv_radius
        hat = jnp.concatenate([kr * sr + ki * si, kr * si - ki * sr], axis=0)
        hi, lo = split_hi_lo(hat)
        ih, il = inv_ref[0], inv_ref[1]
        mid[n] = dot(ih, hi) + (dot(il, hi) + dot(ih, lo))
        return carry

    lax.fori_loop(0, outer // 2, middle, 0)

    def backward(t, carry):
        _, _, re_at, im_at = place(t)
        h = t // out_chunks
        at = pl.ds(pl.multiple_of((t % out_chunks) * step, step), step)
        points = []
        for n in range(outer):
            c = tw_ref[re_at, n : n + 1]
            s = tw_ref[re_at, outer + n : outer + n + 1]
            re = mid[n // 2, re_at, lanes(n)]
            im = mid[n // 2, im_at, lanes(n)]
            points.append((re * c + im * s, im * c - re * s))
        for a, (re, im) in enumerate(fft_list(points, 1)):
            out_ref[a * out_per + h, at, :LANES] = re.astype(jnp.bfloat16)
            out_ref[a * out_per + h, at, LANES:] = im.astype(jnp.bfloat16)
        return carry

    lax.fori_loop(0, inner // step, backward, 0)


def spectral_kernel(
    even_ref, odd_ref, tw_ref, fwd_ref, inv_ref, back_even_ref, back_odd_ref,
    cols, results, mid, fwd_send, fwd_recv, back_send, back_recv, *, total_cols, outer_cols
):
    tile_count = lax.axis_size("col")
    devices = tile_count * lax.axis_size("blk")
    me = lax.axis_index("blk") * tile_count + lax.axis_index("col")
    group = devices // 2
    side, member = me // group, me % group
    sources = (even_ref, odd_ref)
    backs = (back_even_ref, back_odd_ref)

    def place(device):
        return (device // tile_count, device % tile_count)

    barrier = pltpu.get_barrier_semaphore()

    def greet(k, carry):
        pl.semaphore_signal(
            barrier, inc=1, device_id=place((me + k) % devices), device_id_type=MESH
        )
        return carry

    lax.fori_loop(1, devices, greet, 0)
    pl.semaphore_wait(barrier, devices - 1)

    def forward(j, k):
        to = (member + k) % group
        return pltpu.make_async_remote_copy(
            src_ref=sources[j].at[to],
            dst_ref=cols.at[j, member],
            send_sem=fwd_send.at[j, k],
            recv_sem=fwd_recv.at[j, k],
            device_id=place(side * group + to),
            device_id_type=MESH,
        )

    def backward(j, k):
        to = (me + k) % devices
        return pltpu.make_async_remote_copy(
            src_ref=results.at[j, to],
            dst_ref=backs[j].at[me],
            send_sem=back_send.at[j, k],
            recv_sem=back_recv.at[j, k],
            device_id=place(to),
            device_id_type=MESH,
        )

    def every(copy, j, count, act):
        def one(k, carry):
            act(copy(j, k))
            return carry

        lax.fori_loop(1, count, one, 0)

    for j in range(2):
        every(forward, j, group, lambda c: c.start())
    for j in range(2):
        cols[j, member] = sources[j][member]
    for j in range(2):
        every(forward, j, group, lambda c: c.wait_recv())
        cols_transform(
            cols.at[j], tw_ref, fwd_ref, inv_ref, results.at[j], mid,
            4 * member + 2 * side + j, total_cols, outer_cols,
        )
        every(backward, j, devices, lambda c: c.start())
        backs[j][me] = results[j, me]
    for j in range(2):
        every(backward, j, devices, lambda c: c.wait_recv())
    for j in range(2):
        every(forward, j, group, lambda c: c.wait_send())
        every(backward, j, devices, lambda c: c.wait_send())


def back_matmul(in_ref, table_ref, mid):
    half, rows, _ = in_ref.shape
    group = math.gcd(half, 4)

    def matmul(g, carry):
        at = pl.ds(g * group, group)
        data = in_ref[at].reshape(group * rows, 2 * LANES)
        res = dot(data, table_ref[0]) + dot(data, table_ref[1])
        mid[at] = res.reshape(group, rows, 2 * LANES)
        return carry

    lax.fori_loop(0, half // group, matmul, 0)


def half_points(mid, tw_ref, at, parity):
    half = mid.shape[0]
    points = []
    for n in range(half):
        k = 2 * n + parity
        p = n % 2 * (half // 2) + n // 2
        c = tw_ref[k : k + 1, :]
        s = tw_ref[2 * half + k : 2 * half + k + 1, :]
        re = mid[p, at, :LANES]
        im = mid[p, at, LANES:]
        points.append((re * c + im * s, im * c - re * s))
    return fft_list(points, 1)


def back_even_kernel(in_ref, tw_ref, table_ref, out_ref, mid):
    back_matmul(in_ref, table_ref, mid)

    def chunk(rc, carry):
        at = pl.ds(pl.multiple_of(rc * 8, 8), 8)
        for a, (re, im) in enumerate(half_points(mid, tw_ref, at, 0)):
            out_ref[a, at, :LANES] = re
            out_ref[a, at, LANES:] = im
        return carry

    lax.fori_loop(0, in_ref.shape[1] // 8, chunk, 0)


def back_odd_kernel(in_ref, even_ref, tw_ref, table_ref, e_ref, b_ref, mid):
    back_matmul(in_ref, table_ref, mid)
    half = in_ref.shape[0]

    def chunk(rc, carry):
        at = pl.ds(pl.multiple_of(rc * 8, 8), 8)
        for a, (r, i) in enumerate(half_points(mid, tw_ref, at, 1)):
            c, s = math.cos(math.pi * a / half), math.sin(math.pi * a / half)
            tr, ti = r * c - i * s, r * s + i * c
            er, ei = even_ref[a, at, :LANES], even_ref[a, at, LANES:]
            low = slice(a * LANES, (a + 1) * LANES)
            high = slice((half + a) * LANES, (half + a + 1) * LANES)
            e_ref[at, low] = er + tr
            b_ref[at, low] = ei + ti
            e_ref[at, high] = er - tr
            b_ref[at, high] = ei - ti
        return carry

    lax.fori_loop(0, in_ref.shape[1] // 8, chunk, 0)


def vmem(count):
    return [pl.BlockSpec(memory_space=pltpu.VMEM)] * count


def smem():
    return pl.BlockSpec(memory_space=pltpu.SMEM)


def params():
    return pltpu.CompilerParams(vmem_limit_bytes=VMEM_BYTES)


def cost():
    return pl.CostEstimate(flops=4 * 10**9, bytes_accessed=8 * 2**20, transcendentals=0)


def exchange(x, groups=None):
    return lax.all_to_all(
        x, ("blk", "col"), split_axis=0, concat_axis=0, axis_index_groups=groups, tiled=True
    )


def fast_local(pixel_row, pixel_col, strip_of_span, shear_one, shear_two, weight):
    tile_count = lax.axis_size("col")
    devices = tile_count * lax.axis_size("blk")
    me = lax.axis_index("blk") * tile_count + lax.axis_index("col")
    spans, gal = pixel_row.shape
    depth = spans // devices
    rows = SLAB // tile_count
    total_rows = rows * devices
    total_cols = TILE_COLS * tile_count
    outer_x = total_cols // LANES
    outer_y = total_rows // LANES
    f32, bf16 = jnp.float32, jnp.bfloat16

    packed = pl.pallas_call(
        lambda *refs: pack_kernel(*refs, depth=depth),
        out_shape=jax.ShapeDtypeStruct((2 * spans, CHANNELS * gal), bf16),
        in_specs=vmem(6),
        out_specs=vmem(1)[0],
        compiler_params=params(),
        name="pack",
    )(pixel_row, pixel_col, strip_of_span, shear_one, shear_two, weight)
    mine = exchange(packed)
    group_size = devices // 2
    side, member = me // group_size, me % group_size
    groups = [[h * group_size + m for m in range(group_size)] for h in range(2)]
    tile_blocks = TILE_COLS // SUBC
    position = mine[:, 5 * gal].astype(jnp.int32)
    arrival = jnp.arange(2 * spans, dtype=jnp.int32)
    tile = arrival // (2 * depth) % tile_count
    block = tile * tile_blocks + position % tile_blocks
    band = arrival % (2 * depth) // depth * (rows // BAND) + position // tile_blocks

    tw_x = jnp.asarray(np.concatenate(np_twiddle(outer_x, LANES, -1), 0))
    c, s = np_twiddle(outer_y, LANES, -1)
    tw_y = np.zeros((LANES, max(LANES, 2 * outer_y)), np.float32)
    tw_y[:, :outer_y] = c.T
    tw_y[:, outer_y : 2 * outer_y] = s.T
    half = devices
    part = jax.ShapeDtypeStruct((group_size, 2 * rows, 2 * LANES), bf16)
    pre, side_tw = side_tables(outer_x)
    spectra = pl.pallas_call(
        rows_kernel,
        out_shape=[part, part],
        in_specs=[smem()] * 4 + vmem(3),
        out_specs=vmem(2),
        scratch_shapes=[
            pltpu.VMEM((2 * spans, CHANNELS * gal), f32),
            pltpu.VMEM((3, outer_x, 2 * rows, LANES), f32),
            pltpu.VMEM((outer_x // 2, 2 * rows, 2 * LANES), f32),
        ],
        compiler_params=params(),
        name="rows",
    )(
        block,
        band,
        jnp.full((1,), side, jnp.int32),
        jnp.asarray(pre),
        mine,
        jnp.asarray(side_tw),
        jnp.asarray(np_real_form(LANES, -1, 1.0, False)),
    )
    tw_y = jnp.asarray(tw_y)
    fwd_y = jnp.asarray(np_real_form(LANES, -1, 1.0, True))
    inv_y = jnp.asarray(np_real_form(LANES, 1, 1.0 / total_rows, True))
    inv_x = jnp.asarray(np_real_form(LANES, 1, 1.0 / total_cols, False))
    dma = pltpu.SemaphoreType.DMA
    back = pl.pallas_call(
        lambda *refs: spectral_kernel(*refs, total_cols=total_cols, outer_cols=outer_x),
        out_shape=[jax.ShapeDtypeStruct((devices, rows, 2 * LANES), bf16)] * 2,
        in_specs=vmem(5),
        out_specs=vmem(2),
        scratch_shapes=[
            pltpu.VMEM((2, group_size, 2 * rows, 2 * LANES), bf16),
            pltpu.VMEM((2, devices, rows, 2 * LANES), bf16),
            pltpu.VMEM((outer_y // 2, 2 * LANES, 2 * LANES), f32),
            dma((2, group_size)),
            dma((2, group_size)),
            dma((2, devices)),
            dma((2, devices)),
        ],
        compiler_params=pltpu.CompilerParams(
            vmem_limit_bytes=VMEM_BYTES, collective_id=1, has_side_effects=True
        ),
        name="spectral",
    )(spectra[0], spectra[1], tw_y, fwd_y, inv_y)
    scratch = [pltpu.VMEM((half, rows, 2 * LANES), f32)]
    even = pl.pallas_call(
        back_even_kernel,
        out_shape=jax.ShapeDtypeStruct((half, rows, 2 * LANES), f32),
        in_specs=vmem(3),
        out_specs=vmem(1)[0],
        scratch_shapes=scratch,
        compiler_params=params(),
        cost_estimate=cost(),
        name="back_even",
    )(back[0], tw_x, inv_x)
    return tuple(
        pl.pallas_call(
            back_odd_kernel,
            out_shape=[jax.ShapeDtypeStruct((rows, total_cols), f32)] * 2,
            in_specs=vmem(4),
            out_specs=vmem(2),
            scratch_shapes=scratch,
            compiler_params=params(),
            name="back_odd",
        )(back[1], even, tw_x, inv_x)
    )


def local(*args):
    tile_count = lax.axis_size("col")
    devices = tile_count * lax.axis_size("blk")
    if TILE_COLS * tile_count // LANES == 2 * devices:
        return fast_local(*args)
    return generic_local(*args)


def solution(mesh):
    placed = (
        P(("blk", "col"), None),
        P(("blk", "col"), None),
        P(("blk", "col"), None),
        P(("blk", "col"), None),
        P(("blk", "col"), None),
        P(("blk", "col"), None),
    )
    return jax.shard_map(
        local,
        mesh=mesh,
        in_specs=placed,
        out_specs=(P(("blk", "col"), None), P(("blk", "col"), None)),
        check_vma=False,
    )
```
